128 devices in a mesh: row: 32 (over y, x, core), col: 4 (over z).
Axes of the slice: x: 4, y: 4, z: 4, core: 2. Of those that a mesh axis runs over, the one named last changes fastest.
Arguments:
- coeffs: bfloat16 [6144, 4096], P('row', 'col'), may hold values from -0.00390625 to 0.00390625
- occupation: float32 [4096], P('col'), may hold values from 0.5 to 2
- basis_on_grid: bfloat16 [1280, 512, 512], P('row'), may hold values from -6 to 6
- basis_map: int32 [1280, 512], P('row'), may hold values from 0 to 6143, as said below
- basis_count: int32 [1280], P('row'), may hold values from 256 to 512
- batch_atom: int32 [1280], P('row'), may hold values from 0 to 63
- harmonics: float32 [1280, 49, 512], P('row'), may hold values from -0.25 to 0.25
Outputs:
- density: float32 [1280, 512], P('row', 'col')
- moments: float32 [64, 49], replicated
The draws below stay inside these ranges and needn't reach their ends.
Inputs may be any that keep to these rules, and one draw needn't show every extreme that they name: `basis_map`: the slots of one batch name distinct basis functions. With R = 192 and o = b // 40, batch b names only basis functions q * R + (o * 96 + w) mod R with 0 <= q < 32 and 0 <= w < 96.
All inputs are finite; a program needn't handle non-finite values.
Results may differ from the reference program's by a relative error of at most 0.0003.
Values may be sent and summed in bfloat16 or wider, within the bound.
A program may use at most 192 MiB of HBM per device.

```python
import jax
import jax.numpy as jnp
from jax import lax

NB = 6144
NOCC = 4096
SLOTS = 512
WIN = 96
POINTS = 512
LM = 49
NATOM = 64
BD = 40
BATCHES = 1280


def draw_basis_map(key, part):
    owners = BATCHES // BD
    shard = NB // owners
    keys = jax.random.split(jax.random.fold_in(key, 7), BATCHES)
    chosen = jax.vmap(lambda one: jax.random.permutation(one, WIN * owners))(keys)[:, :SLOTS]
    chosen = chosen.astype(jnp.int32)
    source = chosen // WIN
    offset = chosen % WIN
    owner = jnp.arange(BATCHES, dtype=jnp.int32) // BD
    local = jnp.mod(owner[:, None] * WIN + offset, shard)
    return (source * shard + local).astype(jnp.int32)


def set_ends(values, own_key, low, high):
    longest = values.shape.index(max(values.shape))
    spots = []
    for shift in (0, 1):
        where = [jax.random.randint(jax.random.fold_in(own_key, axis), (), 0, length) for axis, length in enumerate(values.shape)]
        where[longest] = (where[longest] + shift) % values.shape[longest]
        spots.append(tuple(where))
    return values.at[spots[0]].set(low).at[spots[1]].set(high)


def block_scale(own_key, extent, cuts, smallest, largest):
    gain, own = 1.0, jax.random.fold_in(own_key, 6)
    for position, shards_of in cuts:
        heights = jnp.exp(jax.random.uniform(jax.random.fold_in(own, position), (shards_of,), jnp.float32, smallest / len(cuts), largest / len(cuts)))
        gain = gain * jnp.repeat(heights, extent[position] // shards_of).reshape([-1 if axis == position else 1 for axis in range(len(extent))])
    return gain


def centred(rng, extent, deviation, limit, pieces=(), held_as=jnp.bfloat16):
    factor_of = block_scale(rng, extent, pieces, -0.22, 0.18) if pieces else 1.0
    entries = jax.random.normal(rng, extent, jnp.float32) * deviation * factor_of
    return jnp.minimum(jnp.maximum(entries, -limit), limit).astype(held_as)


def setup_inputs(seed: int = 0) -> dict:
    seeds = jax.random.split(jax.random.key(seed), 8)
    return {
        "coeffs": centred(seeds[0], (NB, NOCC), (SLOTS * NOCC) ** -0.5, 0.00390625, ((0, 32), (1, 4))),
        "occupation": jnp.clip(0.5 + 1.5 * jax.random.uniform(seeds[1], (NOCC,), jnp.float32) ** block_scale(seeds[1], (NOCC,), ((0, 4),), -0.2, 0.2), 0.5, 2.0),
        "basis_on_grid": centred(seeds[2], (BATCHES, POINTS, SLOTS), 1.0, 6.0, ((0, 32),)),
        "basis_map": draw_basis_map(jax.random.fold_in(seeds[7], 71), 0),
        "basis_count": set_ends(jax.random.randint(seeds[4], (BATCHES,), SLOTS // 2, SLOTS + 1), jax.random.fold_in(seeds[4], 1), SLOTS // 2, SLOTS).astype(jnp.int32),
        "batch_atom": set_ends(jax.random.randint(seeds[5], (BATCHES,), 0, NATOM), jax.random.fold_in(seeds[5], 1), 0, NATOM - 1).astype(jnp.int32),
        "harmonics": centred(seeds[6], (BATCHES, LM, POINTS), POINTS ** -0.5, 0.25, ((0, 32),), jnp.float32),
    }


def reference(coeffs, occupation, basis_on_grid, basis_map, basis_count, batch_atom, harmonics):
    slot_ids = jnp.arange(SLOTS, dtype=jnp.int32)

    def one_batch(items):
        values, indices, count = items
        selected = jnp.take(coeffs, indices, axis=0)
        keep = slot_ids < count
        masked = jnp.where(keep[None, :], values, jnp.zeros_like(values))
        orbital = jnp.dot(masked, selected, preferred_element_type=jnp.float32)
        return jnp.sum(occupation[None, :] * orbital * orbital, axis=1)

    density = lax.map(one_batch, (basis_on_grid, basis_map, basis_count))
    local_moment = jnp.einsum("blp,bp->bl", harmonics, density, precision=lax.Precision.HIGHEST)
    member = (batch_atom[:, None] == jnp.arange(NATOM, dtype=jnp.int32)[None, :]).astype(jnp.float32)
    moments = jnp.dot(member.T, local_moment, precision=lax.Precision.HIGHEST)
    return density, moments
```

```python
import jax
import jax.numpy as jnp
from jax import lax
from jax.experimental import pallas as pl
from jax.experimental.pallas import tpu as pltpu
from jax.sharding import Mesh, PartitionSpec as P

NATOM = 64
WIN = 96
GROUPS = 8
LANES = 128


def density_kernel(idx_ref, w_ref, occ_ref, m_ref, out_ref, wide, even, odd, acc):
    step = pl.program_id(0)
    slots = m_ref.shape[2]
    stride = slots + 1
    rows = w_ref.shape[0]

    def pick(into, batch, low, high):
        for s in range(low, high):
            at = pl.multiple_of(idx_ref[batch * slots + s], GROUPS)
            into[pl.ds(s, GROUPS, stride=stride), :] = wide[pl.ds(at, GROUPS), :]

    def multiply(held, which, tile):
        right = jnp.concatenate(
            [held[pl.ds((2 * tile + h) * stride, slots), :].astype(jnp.bfloat16) for h in range(2)], axis=1
        )
        orbital = jnp.dot(m_ref[which], right, preferred_element_type=jnp.float32)
        left_half, right_half = orbital[:, :LANES], orbital[:, LANES:]
        term = (
            left_half * left_half * occ_ref[2 * tile : 2 * tile + 1, :]
            + right_half * right_half * occ_ref[2 * tile + 1 : 2 * tile + 2, :]
        )
        acc[which] = term if tile == 0 else acc[which] + term

    @pl.when(step == 0)
    def _():
        for r in range(0, rows, 512):
            wide[pl.ds(r, 512), :] = w_ref[pl.ds(r, 512), :].astype(jnp.float32)
        wide[pl.ds(rows, GROUPS), :] = jnp.zeros((GROUPS, LANES), jnp.float32)
        pick(even, 0, 0, slots)

    tiles = GROUPS // 2
    for which in range(2):
        held, into = (even, odd) if which == 0 else (odd, even)
        for tile in range(tiles):
            pick(into, 2 * step + which + 1, tile * slots // tiles, (tile + 1) * slots // tiles)
            multiply(held, which, tile)
    for which in range(2):
        out_ref[0, pl.ds(which, 1), :] = jnp.sum(acc[which].T, axis=0, keepdims=True)


def partial_densities(idx, window, occ, basis_on_grid):
    batches, points, slots = basis_on_grid.shape
    rows = window.shape[0]
    out = pl.pallas_call(
        density_kernel,
        grid=(batches // 2,),
        in_specs=[
            pl.BlockSpec(memory_space=pltpu.SMEM),
            pl.BlockSpec((rows, LANES), lambda i: (0, 0), pipeline_mode=pl.Buffered(1)),
            pl.BlockSpec((GROUPS, LANES), lambda i: (0, 0)),
            pl.BlockSpec((2, points, slots), lambda i: (i, 0, 0)),
        ],
        out_specs=pl.BlockSpec((1, 2, points), lambda i: (i, 0, 0)),
        out_shape=jax.ShapeDtypeStruct((batches // 2, 2, points), jnp.float32),
        scratch_shapes=[
            pltpu.VMEM((rows + GROUPS, LANES), jnp.float32),
            pltpu.VMEM(((slots + 1) * GROUPS + 8, LANES), jnp.float32),
            pltpu.VMEM(((slots + 1) * GROUPS + 8, LANES), jnp.float32),
            pltpu.VMEM((2, points, LANES), jnp.float32),
        ],
        compiler_params=pltpu.CompilerParams(vmem_limit_bytes=60 * 2**20),
        cost_estimate=pl.CostEstimate(
            flops=2 * batches * points * slots * GROUPS * LANES, bytes_accessed=batches * points * slots * 2, transcendentals=0
        ),
    )(idx, window, occ, basis_on_grid)
    return out.reshape(batches, points)


def shards(coeffs, occupation, basis_on_grid, basis_map, basis_count, batch_atom, harmonics):
    batches, points, slots = basis_on_grid.shape
    parity = lax.axis_index("core")
    shard = coeffs.shape[0]
    halves = coeffs.reshape(2, WIN, GROUPS, LANES)
    mine = lax.dynamic_index_in_dim(halves, parity, 0, keepdims=False)
    other = lax.dynamic_index_in_dim(halves, 1 - parity, 0, keepdims=False)
    theirs = lax.ppermute(other, "core", [(0, 1), (1, 0)])
    first = jnp.where(parity == 0, mine, theirs)
    second = jnp.where(parity == 0, theirs, mine)
    both = jnp.concatenate([first, second], axis=0).reshape(2 * WIN * GROUPS, LANES)
    window = lax.all_gather(both, "chip", axis=0, tiled=True)
    place = (basis_map // shard) * WIN + basis_map % shard - parity * WIN
    slot_ids = lax.broadcasted_iota(jnp.int32, (batches, slots), 1)
    place = jnp.where(slot_ids < basis_count[:, None], place, window.shape[0] // GROUPS) * GROUPS
    idx = jnp.concatenate([place.reshape(-1), place[0]])
    part = partial_densities(idx, window, occupation.reshape(GROUPS, LANES), basis_on_grid)
    zs = lax.axis_size("col")
    share = points // zs
    pieces = lax.all_to_all(part.reshape(batches, zs, share).transpose(1, 0, 2), "col", split_axis=0, concat_axis=0, tiled=True)
    density = jnp.sum(pieces, axis=0)
    mine_harm = lax.dynamic_slice_in_dim(harmonics, lax.axis_index("col") * share, share, 2)
    local_moment = jnp.einsum("blp,bp->bl", mine_harm, density, precision=lax.Precision.HIGHEST)
    atom_ids = lax.broadcasted_iota(jnp.int32, (batches, NATOM), 1)
    member = (batch_atom[:, None] == atom_ids).astype(jnp.float32)
    atom_part = jnp.dot(member.T, local_moment, precision=lax.Precision.HIGHEST)
    moments = lax.psum(atom_part, ("chip", "core", "col"))
    return density, moments


def solution(mesh):
    rows, cols = mesh.devices.shape
    split = Mesh(mesh.devices.reshape(rows // 2, 2, cols), ("chip", "core", "col"))
    row = ("chip", "core")
    placed = (
        P(row, "col"),
        P("col"),
        P(row, None, None),
        P(row, None),
        P(row),
        P(row),
        P(row, None, None),
    )
    return jax.shard_map(shards, mesh=split, in_specs=placed, out_specs=(P(row, "col"), P()), check_vma=False)
```

```python
import jax
import jax.numpy as jnp
from jax import lax
from jax.experimental import pallas as pl
from jax.experimental.pallas import tpu as pltpu
from jax.sharding import PartitionSpec as P

NATOM = 64
SIDE = 4
MESH = pl.DeviceIdType.MESH
WIN = 96
GROUPS = 8
LANES = 128


def place_of(row):
    return row // (2 * SIDE), (row // 2) % SIDE, row % 2


def window_kernel(coeffs_ref, out_ref, staged, other, send_sem, recv_sem):
    me = lax.axis_index("row")
    col = lax.axis_index("col")
    y, x, core = place_of(me)
    block = WIN * GROUPS

    def row_of(dy, dx):
        return (lax.rem(y + dy + SIDE, SIDE) * SIDE + lax.rem(x + dx + SIDE, SIDE)) * 2 + core

    def turned(first, second, turn):
        return first * turn + second * (1 - turn), first * (1 - turn) + second * turn

    def rows_of(first, second, turn, half):
        q = row_of(*turned(first, second, turn)) - core + turn
        if half is None:
            return pl.ds(pl.multiple_of(q * block, block), block)
        return pl.ds(pl.multiple_of(q * block + half * (block // 2), block // 2), block // 2)

    def copy(turn, number, at, to, half=None):
        here = out_ref.at[rows_of(*at, turn, half)]
        sem = turn * 20 + number
        return pltpu.make_async_remote_copy(
            src_ref=here, dst_ref=here, send_sem=send_sem.at[sem], recv_sem=recv_sem.at[sem],
            device_id=(row_of(*turned(*to, turn)), col), device_id_type=MESH,
        )

    sent = []

    def send(turn, number, at, to, half=None):
        one = copy(turn, number, at, to, half)
        one.start()
        sent.append(one)

    def arrive(turn, number, at, half=None):
        copy(turn, number, at, (0, 1), half).wait_recv()

    for j in range(GROUPS):
        staged[pl.ds(j, 2 * WIN, stride=GROUPS), :] = coeffs_ref[:, j * LANES : (j + 1) * LANES].astype(jnp.float32)
    mine = pl.multiple_of(core * block, block)
    theirs = pl.multiple_of((1 - core) * block, block)
    other[...] = staged[pl.ds(theirs, block), :].astype(jnp.bfloat16)
    own_rows = rows_of(0, 0, core, None)
    out_ref[own_rows, :] = staged[pl.ds(mine, block), :].astype(jnp.bfloat16)

    barrier = pltpu.get_barrier_semaphore()
    partner = me - core + (1 - core)
    near = [partner, row_of(0, 1), row_of(0, -1), row_of(1, 0), row_of(-1, 0)]
    for row in near:
        pl.semaphore_signal(barrier, inc=1, device_id=(row, col), device_id_type=MESH)
    pl.semaphore_wait(barrier, len(near))

    swap = pltpu.make_async_remote_copy(
        src_ref=other, dst_ref=out_ref.at[own_rows], send_sem=send_sem.at[40], recv_sem=recv_sem.at[40],
        device_id=(partner, col), device_id_type=MESH,
    )
    swap.start()
    a, b = core, 1 - core
    blocks = [(0, 0), (-1, 0), (1, 0), (2, 0)]

    def outward(turn):
        send(turn, 0, (0, 0), (1, 0))
        send(turn, 1, (0, 0), (-1, 0))
        across(turn, 0)

    def across(turn, k):
        send(turn, 4 + 2 * k, blocks[k], (0, 1))
        send(turn, 5 + 2 * k, blocks[k], (0, -1))

    def first_hop(turn):
        arrive(turn, 0, (-1, 0))
        send(turn, 2, (-1, 0), (1, 0), 0)
        arrive(turn, 1, (1, 0))
        send(turn, 3, (1, 0), (-1, 0), 1)
        across(turn, 1)
        across(turn, 2)

    def second_hop(turn):
        arrive(turn, 2, (2, 0), 0)
        arrive(turn, 3, (2, 0), 1)
        across(turn, 3)

    def onward(turn, k):
        f = blocks[k][0]
        arrive(turn, 4 + 2 * k, (f, -1))
        send(turn, 12 + 2 * k, (f, -1), (0, 1), 0)
        arrive(turn, 5 + 2 * k, (f, 1))
        send(turn, 13 + 2 * k, (f, 1), (0, -1), 1)

    outward(a)
    pltpu.make_async_remote_copy(
        src_ref=other, dst_ref=out_ref.at[rows_of(0, 0, b, None)], send_sem=send_sem.at[40], recv_sem=recv_sem.at[40],
        device_id=(partner, col), device_id_type=MESH,
    ).wait_recv()
    outward(b)
    first_hop(a)
    onward(a, 0)
    first_hop(b)
    onward(b, 0)
    second_hop(a)
    second_hop(b)
    for k in (1, 2, 3):
        onward(a, k)
        onward(b, k)
    for turn in (a, b):
        for k in range(4):
            f = blocks[k][0]
            arrive(turn, 12 + 2 * k, (f, 2), 0)
            arrive(turn, 13 + 2 * k, (f, 2), 1)
    swap.wait_send()
    for one in sent:
        one.wait_send()


def gather_window(coeffs):
    rows = 2 * SIDE * SIDE * WIN * GROUPS
    return pl.pallas_call(
        window_kernel,
        out_shape=jax.ShapeDtypeStruct((rows, LANES), jnp.bfloat16),
        in_specs=[pl.BlockSpec(memory_space=pltpu.VMEM)],
        out_specs=pl.BlockSpec(memory_space=pltpu.VMEM),
        scratch_shapes=[
            pltpu.VMEM((2 * WIN * GROUPS, LANES), jnp.float32),
            pltpu.VMEM((WIN * GROUPS, LANES), jnp.bfloat16),
            pltpu.SemaphoreType.DMA((41,)),
            pltpu.SemaphoreType.DMA((41,)),
        ],
        compiler_params=pltpu.CompilerParams(collective_id=0, has_side_effects=True, vmem_limit_bytes=16 * 2**20),
    )(coeffs)


def total_kernel(part_ref, atoms_ref, density_ref, moments_ref, parts, column, line, plane, square, send_sem, recv_sem):
    me = lax.axis_index("row")
    z = lax.axis_index("col")
    y, x, core = place_of(me)
    pairs = [(dz, dc) for dz in range(SIDE) for dc in range(2) if (dz, dc) != (0, 0)]

    def column_device(dz, dc):
        return me - core + lax.rem(core + dc, 2), lax.rem(z + dz, SIDE)

    def line_device(d):
        return (y * SIDE + lax.rem(x + d, SIDE)) * 2 + core, z

    def plane_device(d):
        return (lax.rem(y + d, SIDE) * SIDE + x) * 2 + core, z

    barrier = pltpu.get_barrier_semaphore()
    near = [column_device(*p) for p in pairs] + [line_device(d) for d in (1, 2, 3)] + [plane_device(d) for d in (1, 2, 3)]
    for device in near:
        pl.semaphore_signal(barrier, inc=1, device_id=device, device_id_type=MESH)
    pl.semaphore_wait(barrier, len(near))

    def remote(src, dst, number, device):
        return pltpu.make_async_remote_copy(
            src_ref=src, dst_ref=dst, send_sem=send_sem.at[number], recv_sem=recv_sem.at[number],
            device_id=device, device_id_type=MESH,
        )

    slot = z * 2 + core
    sends = []
    for n, (dz, dc) in enumerate(pairs):
        sends.append(remote(atoms_ref, column.at[slot], n, column_device(dz, dc)))
    for dz in (1, 2, 3):
        sends.append(remote(part_ref.at[lax.rem(z + dz, SIDE)], parts.at[z], 6 + dz, column_device(dz, 0)))
    for one in sends:
        one.start()
    column[slot] = atoms_ref[...]
    parts[z] = part_ref[z]
    for n, (dz, dc) in enumerate(pairs):
        source = lax.rem(z - dz + SIDE, SIDE) * 2 + lax.rem(core + dc, 2)
        remote(atoms_ref, column.at[source], n, column_device(dz, dc)).wait_recv()
    here = column[0]
    for s in range(1, 2 * SIDE):
        here = here + column[s]
    line[x] = here
    lines = [remote(line.at[x], line.at[x], 9 + d, line_device(d)) for d in (1, 2, 3)]
    for one in lines:
        one.start()
    for dz in (1, 2, 3):
        source = lax.rem(z - dz + SIDE, SIDE)
        remote(part_ref.at[0], parts.at[source], 6 + dz, column_device(dz, 0)).wait_recv()
    density_ref[...] = parts[0] + parts[1] + parts[2] + parts[3]
    for d in (1, 2, 3):
        source = lax.rem(x - d + SIDE, SIDE)
        remote(line.at[source], line.at[source], 9 + d, line_device(d)).wait_recv()
    plane[y] = line[0] + line[1] + line[2] + line[3]
    planes = [remote(plane.at[y], plane.at[y], 12 + d, plane_device(d)) for d in (1, 2, 3)]
    for one in planes:
        one.start()
    for d in (1, 2, 3):
        source = lax.rem(y - d + SIDE, SIDE)
        remote(plane.at[source], plane.at[source], 12 + d, plane_device(d)).wait_recv()
    square[...] = jnp.zeros_like(square)
    square[pl.ds(0, plane.shape[1]), :] = plane[0] + plane[1] + plane[2] + plane[3]
    moments_ref[...] = square[...].T[: moments_ref.shape[0], : moments_ref.shape[1]]
    for one in sends + lines + planes:
        one.wait_send()


def totals(part, atoms, components):
    zs, batches, share = part.shape
    kept = atoms.shape[0]
    return pl.pallas_call(
        total_kernel,
        out_shape=(
            jax.ShapeDtypeStruct((batches, share), jnp.float32),
            jax.ShapeDtypeStruct((NATOM, components), jnp.float32),
        ),
        in_specs=[pl.BlockSpec(memory_space=pltpu.VMEM)] * 2,
        out_specs=(pl.BlockSpec(memory_space=pltpu.VMEM), pl.BlockSpec(memory_space=pltpu.VMEM)),
        scratch_shapes=[
            pltpu.VMEM((zs, batches, share), jnp.float32),
            pltpu.VMEM((2 * SIDE, kept, LANES), jnp.float32),
            pltpu.VMEM((SIDE, kept, LANES), jnp.float32),
            pltpu.VMEM((SIDE, kept, LANES), jnp.float32),
            pltpu.VMEM((LANES, LANES), jnp.float32),
            pltpu.SemaphoreType.DMA((16,)),
            pltpu.SemaphoreType.DMA((16,)),
        ],
        compiler_params=pltpu.CompilerParams(collective_id=1, has_side_effects=True, vmem_limit_bytes=16 * 2**20),
    )(part, atoms)


def density_kernel(idx_ref, atom_ref, w_ref, occ_ref, m_ref, harm_ref, out_ref, sums_ref, wide, even, odd, acc):
    step = pl.program_id(0)
    slots = m_ref.shape[2]
    stride = slots + 1
    rows = w_ref.shape[0]

    def pick(into, batch, low, high):
        for s in range(low, high):
            at = pl.multiple_of(idx_ref[batch * slots + s], GROUPS)
            into[pl.ds(s, GROUPS, stride=stride), :] = wide[pl.ds(at, GROUPS), :]

    def multiply(held, which, tile):
        right = jnp.concatenate(
            [held[pl.ds((2 * tile + h) * stride, slots), :].astype(jnp.bfloat16) for h in range(2)], axis=1
        )
        orbital = jnp.dot(m_ref[which], right, preferred_element_type=jnp.float32)
        left_half, right_half = orbital[:, :LANES], orbital[:, LANES:]
        term = (
            left_half * left_half * occ_ref[2 * tile : 2 * tile + 1, :]
            + right_half * right_half * occ_ref[2 * tile + 1 : 2 * tile + 2, :]
        )
        acc[which] = term if tile == 0 else acc[which] + term

    @pl.when(step == 0)
    def _():
        for r in range(0, rows, 512):
            wide[pl.ds(r, 512), :] = w_ref[pl.ds(r, 512), :].astype(jnp.float32)
        wide[pl.ds(rows, GROUPS), :] = jnp.zeros((GROUPS, LANES), jnp.float32)
        sums_ref[...] = jnp.zeros_like(sums_ref)
        pick(even, 0, 0, slots)

    tiles = GROUPS // 2
    for which in range(2):
        held, into = (even, odd) if which == 0 else (odd, even)
        for tile in range(tiles):
            pick(into, 2 * step + which + 1, tile * slots // tiles, (tile + 1) * slots // tiles)
            multiply(held, which, tile)
    atom_ids = lax.broadcasted_iota(jnp.int32, (harm_ref.shape[1], LANES), 1)
    for which in range(2):
        row = jnp.sum(acc[which].T, axis=0, keepdims=True)
        for z in range(out_ref.shape[0]):
            out_ref[z, pl.ds(2 * step + which, 1), :] = row[:, z * LANES : (z + 1) * LANES]
        moment = jnp.sum(harm_ref[which] * row, axis=1, keepdims=True)
        mine = atom_ids == atom_ref[2 * step + which]
        sums_ref[pl.ds(0, harm_ref.shape[1]), :] += jnp.where(mine, moment, 0.0)


def partial_densities(idx, batch_atom, window, occ, basis_on_grid, harmonics):
    batches, points, slots = basis_on_grid.shape
    rows = window.shape[0]
    components = harmonics.shape[1]
    kept = -(-components // 8) * 8
    return pl.pallas_call(
        density_kernel,
        grid=(batches // 2,),
        in_specs=[
            pl.BlockSpec(memory_space=pltpu.SMEM),
            pl.BlockSpec(memory_space=pltpu.SMEM),
            pl.BlockSpec((rows, LANES), lambda i: (0, 0), pipeline_mode=pl.Buffered(1)),
            pl.BlockSpec((GROUPS, LANES), lambda i: (0, 0)),
            pl.BlockSpec((2, points, slots), lambda i: (i, 0, 0)),
            pl.BlockSpec((2, components, points), lambda i: (i, 0, 0)),
        ],
        out_specs=(
            pl.BlockSpec((points // LANES, batches, LANES), lambda i: (0, 0, 0)),
            pl.BlockSpec((kept, LANES), lambda i: (0, 0)),
        ),
        out_shape=(
            jax.ShapeDtypeStruct((points // LANES, batches, LANES), jnp.float32),
            jax.ShapeDtypeStruct((kept, LANES), jnp.float32),
        ),
        scratch_shapes=[
            pltpu.VMEM((rows + GROUPS, LANES), jnp.float32),
            pltpu.VMEM(((slots + 1) * GROUPS + 8, LANES), jnp.float32),
            pltpu.VMEM(((slots + 1) * GROUPS + 8, LANES), jnp.float32),
            pltpu.VMEM((2, points, LANES), jnp.float32),
        ],
        compiler_params=pltpu.CompilerParams(vmem_limit_bytes=60 * 2**20),
        cost_estimate=pl.CostEstimate(
            flops=2 * batches * points * slots * GROUPS * LANES, bytes_accessed=batches * points * slots * 2, transcendentals=0
        ),
    )(idx, batch_atom, window, occ, basis_on_grid, harmonics)


def shards(coeffs, occupation, basis_on_grid, basis_map, basis_count, batch_atom, harmonics):
    batches, points, slots = basis_on_grid.shape
    parity = lax.rem(lax.axis_index("row"), 2)
    shard = coeffs.shape[0]
    window = gather_window(coeffs)
    place = (basis_map // shard) * WIN + basis_map % shard - parity * WIN
    slot_ids = lax.broadcasted_iota(jnp.int32, (batches, slots), 1)
    place = jnp.where(slot_ids < basis_count[:, None], place, window.shape[0] // GROUPS) * GROUPS
    idx = jnp.concatenate([place.reshape(-1), place[0]])
    part, atoms = partial_densities(
        idx, batch_atom, window, occupation.reshape(GROUPS, LANES), basis_on_grid, harmonics
    )
    return totals(part, atoms, harmonics.shape[1])


def solution(mesh):
    placed = (
        P("row", "col"),
        P("col"),
        P("row", None, None),
        P("row", None),
        P("row"),
        P("row"),
        P("row", None, None),
    )
    return jax.shard_map(shards, mesh=mesh, in_specs=placed, out_specs=(P("row", "col"), P()), check_vma=False)
```

```python
import jax
import jax.numpy as jnp
from jax import lax
from jax.experimental import pallas as pl
from jax.experimental.pallas import tpu as pltpu
from jax.sharding import PartitionSpec as P

NATOM = 64
WIN = 96
LANES = 128
SIDE = 4
PASSES = 2
GROUPS = 4
BLOCK = WIN * GROUPS
UNROLL = 4
MESH = pl.DeviceIdType.MESH
OFFSETS = ((0, 0), (-1, 0), (1, 0), (2, 0))
MESSAGES = 20


def message(number):
    if number < 2:
        return (0, 0), (1 - 2 * number, 0), None
    if number < 4:
        return (2 * number - 5, 0), (5 - 2 * number, 0), number - 2
    k, down = (number - 4) // 2 % 4, number % 2
    if number < 12:
        return OFFSETS[k], (0, 1 - 2 * down), None
    return (OFFSETS[k][0], 2 * down - 1), (0, 1 - 2 * down), down


def arrival(number):
    at, to, half = message(number)
    first, second = at[0] - to[0], at[1] - to[1]
    return (2 if first == -2 else first, 2 if second == -2 else second), half


def kernel(
    idx_ref, coeffs_ref, occ_ref, m_ref, harm_hbm, member_ref, density_ref, moments_ref,
    window, staged, other, wide, even, odd, acc, harm, part, parts, column, line, plane,
    send_sem, recv_sem, sum_send, sum_recv, harm_sem,
):
    half_of_states, step = pl.program_id(0), pl.program_id(1)
    steps = pl.num_programs(1)
    me = lax.axis_index("row")
    z = lax.axis_index("col")
    y, x, core = me // (2 * SIDE), (me // 2) % SIDE, me % 2
    slots = m_ref.shape[2]
    rows = window.shape[1]

    def row_of(dy, dx):
        return (lax.rem(y + dy + SIDE, SIDE) * SIDE + lax.rem(x + dx + SIDE, SIDE)) * 2 + core

    def turned(first, second, turn):
        return first * turn + second * (1 - turn), first * (1 - turn) + second * turn

    def rows_at(at, turn, half):
        q = row_of(*turned(*at, turn)) - core + turn
        if half is None:
            return pl.ds(pl.multiple_of(q * BLOCK, BLOCK), BLOCK)
        return pl.ds(pl.multiple_of(q * BLOCK + half * (BLOCK // 2), BLOCK // 2), BLOCK // 2)

    def copy(chunk, turn, number, at, half):
        to = message(number)[1]
        place = window.at[chunk, rows_at(at, turn, half)]
        sem = chunk * 2 * MESSAGES + turn * MESSAGES + number
        return pltpu.make_async_remote_copy(
            src_ref=place, dst_ref=place, send_sem=send_sem.at[sem], recv_sem=recv_sem.at[sem],
            device_id=(row_of(*turned(*to, turn)), z), device_id_type=MESH,
        )

    def outgoing(chunk, turn, number):
        at, _, half = message(number)
        return copy(chunk, turn, number, at, half)

    def send(chunk, turn, *numbers):
        for number in numbers:
            outgoing(chunk, turn, number).start()

    def arrive(chunk, turn, *numbers):
        for number in numbers:
            at, half = arrival(number)
            copy(chunk, turn, number, at, half).wait_recv()

    a, b = core, 1 - core
    partner = me - core + b

    def swap(chunk, turn):
        sem = PASSES * 2 * MESSAGES + chunk
        return pltpu.make_async_remote_copy(
            src_ref=other.at[chunk], dst_ref=window.at[chunk, rows_at((0, 0), turn, None)],
            send_sem=send_sem.at[sem], recv_sem=recv_sem.at[sem], device_id=(partner, z), device_id_type=MESH,
        )

    def outward(chunk, turn):
        send(chunk, turn, 0, 1, 4, 5)

    def first_hop(chunk, turn):
        arrive(chunk, turn, 0)
        send(chunk, turn, 2)
        arrive(chunk, turn, 1)
        send(chunk, turn, 3, 6, 7, 8, 9)

    def second_hop(chunk, turn):
        arrive(chunk, turn, 2, 3)
        send(chunk, turn, 10, 11)

    def onward(chunk, turn, k):
        arrive(chunk, turn, 4 + 2 * k)
        send(chunk, turn, 12 + 2 * k)
        arrive(chunk, turn, 5 + 2 * k)
        send(chunk, turn, 13 + 2 * k)

    def last_arrivals(chunk):
        for turn in (a, b):
            arrive(chunk, turn, *range(12, 20))

    pairs = [(dz, dc) for dz in range(SIDE) for dc in range(2) if (dz, dc) != (0, 0)]

    def column_device(dz, dc):
        return me - core + lax.rem(core + dc, 2), lax.rem(z + dz, SIDE)

    def pick(into, batch, low, high):
        for s in range(low, high):
            into[pl.ds(s * GROUPS, GROUPS), :] = wide[pl.ds(idx_ref[batch * slots + s], GROUPS), :]

    harm_copy = pltpu.make_async_copy(harm_hbm, harm, harm_sem)

    @pl.when((half_of_states == 0) & (step == 0))
    def _():
        harm_copy.start()
        for chunk in range(PASSES):
            for j in range(GROUPS):
                lane = (chunk * GROUPS + j) * LANES
                staged[pl.ds(chunk * 2 * BLOCK + j, 2 * WIN, stride=GROUPS), :] = coeffs_ref[
                    :, lane : lane + LANES
                ].astype(jnp.float32)
            base = chunk * 2 * BLOCK
            other[chunk] = staged[pl.ds(pl.multiple_of(base + b * BLOCK, BLOCK), BLOCK), :].astype(jnp.bfloat16)
            window[chunk, rows_at((0, 0), a, None), :] = staged[
                pl.ds(pl.multiple_of(base + a * BLOCK, BLOCK), BLOCK), :
            ].astype(jnp.bfloat16)
        barrier = pltpu.get_barrier_semaphore()
        near = [column_device(*p) for p in pairs]
        near += [(row_of(0, d), z) for d in (1, 2, 3)] + [(row_of(d, 0), z) for d in (1, 2, 3)]
        for device in near:
            pl.semaphore_signal(barrier, inc=1, device_id=device, device_id_type=MESH)
        pl.semaphore_wait(barrier, len(near))
        swap(0, a).start()
        swap(1, a).start()
        outward(0, a)
        swap(0, b).wait_recv()
        outward(0, b)
        for turn in (a, b):
            first_hop(0, turn)
            onward(0, turn, 0)
        for turn in (a, b):
            second_hop(0, turn)
        for k in (1, 2, 3):
            for turn in (a, b):
                onward(0, turn, k)
        swap(1, b).wait_recv()
        outward(1, a)
        outward(1, b)
        last_arrivals(0)
        part[...] = jnp.zeros_like(part)
        wide[pl.ds(rows, 8), :] = jnp.zeros((8, LANES), jnp.float32)

    @pl.when((half_of_states == 1) & (step == 0))
    def _():
        last_arrivals(1)

    @pl.when(step == 0)
    def _():
        for r in range(0, rows, 512):
            wide[pl.ds(r, 512), :] = window[half_of_states, pl.ds(r, 512), :].astype(jnp.float32)
        pick(even, 0, 0, slots)

    @pl.when(half_of_states == 0)
    def _():
        @pl.when(step == 0)
        def _():
            first_hop(1, a)
            onward(1, a, 0)

        @pl.when(step == 1)
        def _():
            first_hop(1, b)
            onward(1, b, 0)

        @pl.when(step == 2)
        def _():
            second_hop(1, a)
            second_hop(1, b)

        for k in (1, 2, 3):
            @pl.when(step == 2 + k)
            def _():
                onward(1, a, k)
                onward(1, b, k)

    for which in range(UNROLL):
        held, into = (even, odd) if which % 2 == 0 else (odd, even)
        batch = UNROLL * step + which
        pick(into, batch + 1, 0, slots)
        right = jnp.concatenate(
            [held[pl.ds(j, slots, stride=GROUPS), :].astype(jnp.bfloat16) for j in range(GROUPS)], axis=1
        )
        orbital = jnp.dot(m_ref[which], right, preferred_element_type=jnp.float32)
        total = None
        for j in range(GROUPS):
            one = orbital[:, j * LANES : (j + 1) * LANES]
            term = one * one * occ_ref[0, j : j + 1, :]
            total = term if total is None else total + term
        acc[which] = total
        row = jnp.sum(acc[which].T, axis=0, keepdims=True)
        for c in range(SIDE):
            part[c, pl.ds(batch, 1), :] += row[:, c * LANES : (c + 1) * LANES]

    @pl.when((half_of_states == 1) & (step == steps - 1))
    def _():
        def remote(ref, slot, source, number, device):
            return pltpu.make_async_remote_copy(
                src_ref=source, dst_ref=ref.at[slot], send_sem=sum_send.at[number], recv_sem=sum_recv.at[number],
                device_id=device, device_id_type=MESH,
            )

        densities = [
            remote(parts, z, part.at[lax.rem(z + dz, SIDE)], 6 + dz, column_device(dz, 0)) for dz in (1, 2, 3)
        ]
        for one in densities:
            one.start()
        parts[z] = part[z]
        harm_copy.wait()
        lane = lax.broadcasted_iota(jnp.int32, (part.shape[1], LANES), 1)
        local = jnp.zeros((part.shape[1], LANES), jnp.float32)
        for l in range(harm.shape[0]):
            product = harm[l, :, :LANES] * part[0]
            for c in range(1, SIDE):
                product += harm[l, :, c * LANES : (c + 1) * LANES] * part[c]
            local = jnp.where(lane == l, jnp.sum(product, axis=1, keepdims=True), local)
        slot = z * 2 + core
        column[slot] = jnp.dot(
            member_ref[...], local, precision=lax.Precision.HIGHEST, preferred_element_type=jnp.float32
        )
        columns = [remote(column, slot, column.at[slot], n, column_device(*p)) for n, p in enumerate(pairs)]
        for one in columns:
            one.start()
        for dz in (1, 2, 3):
            source = lax.rem(z - dz + SIDE, SIDE)
            remote(parts, source, part.at[0], 6 + dz, column_device(dz, 0)).wait_recv()
        density_ref[...] = parts[0] + parts[1] + parts[2] + parts[3]
        for n, (dz, dc) in enumerate(pairs):
            source = lax.rem(z - dz + SIDE, SIDE) * 2 + lax.rem(core + dc, 2)
            remote(column, source, column.at[source], n, column_device(dz, dc)).wait_recv()
        here = column[0]
        for s in range(1, 2 * SIDE):
            here = here + column[s]
        line[x] = here
        lines = [remote(line, x, line.at[x], 9 + d, (row_of(0, d), z)) for d in (1, 2, 3)]
        for one in lines:
            one.start()
        for d in (1, 2, 3):
            source = lax.rem(x - d + SIDE, SIDE)
            remote(line, source, line.at[source], 9 + d, (row_of(0, d), z)).wait_recv()
        plane[y] = line[0] + line[1] + line[2] + line[3]
        planes = [remote(plane, y, plane.at[y], 12 + d, (row_of(d, 0), z)) for d in (1, 2, 3)]
        for one in planes:
            one.start()
        for d in (1, 2, 3):
            source = lax.rem(y - d + SIDE, SIDE)
            remote(plane, source, plane.at[source], 12 + d, (row_of(d, 0), z)).wait_recv()
        everything = plane[0] + plane[1] + plane[2] + plane[3]
        moments_ref[...] = everything.T[: moments_ref.shape[0], :]
        for one in densities + columns + lines + planes:
            one.wait_send()
        for chunk in range(PASSES):
            swap(chunk, a).wait_send()
            for turn in (a, b):
                for number in range(MESSAGES):
                    outgoing(chunk, turn, number).wait_send()


def shards(coeffs, occupation, basis_on_grid, basis_map, basis_count, batch_atom, harmonics):
    batches, points, slots = basis_on_grid.shape
    components = harmonics.shape[1]
    parity = lax.rem(lax.axis_index("row"), 2)
    shard = coeffs.shape[0]
    rows = 2 * SIDE * SIDE * BLOCK
    place = (basis_map // shard) * WIN + basis_map % shard - parity * WIN
    slot_ids = lax.broadcasted_iota(jnp.int32, (batches, slots), 1)
    place = jnp.where(slot_ids < basis_count[:, None], place * GROUPS, rows)
    idx = jnp.concatenate([place.reshape(-1), place[0]])
    member = (lax.broadcasted_iota(jnp.int32, (NATOM, batches), 0) == batch_atom[None, :]).astype(jnp.float32)
    density, moments = pl.pallas_call(
        kernel,
        grid=(PASSES, batches // UNROLL),
        in_specs=[
            pl.BlockSpec(memory_space=pltpu.SMEM),
            pl.BlockSpec(coeffs.shape, lambda p, i: (0, 0)),
            pl.BlockSpec((1, GROUPS, LANES), lambda p, i: (p, 0, 0)),
            pl.BlockSpec((UNROLL, points, slots), lambda p, i: (i, 0, 0)),
            pl.BlockSpec(memory_space=pl.ANY),
            pl.BlockSpec((NATOM, batches), lambda p, i: (0, 0)),
        ],
        out_specs=(
            pl.BlockSpec((batches, points // SIDE), lambda p, i: (0, 0)),
            pl.BlockSpec((components, NATOM), lambda p, i: (0, 0)),
        ),
        out_shape=(
            jax.ShapeDtypeStruct((batches, points // SIDE), jnp.float32),
            jax.ShapeDtypeStruct((components, NATOM), jnp.float32),
        ),
        scratch_shapes=[
            pltpu.VMEM((PASSES, rows, LANES), jnp.bfloat16),
            pltpu.VMEM((PASSES * 2 * BLOCK, LANES), jnp.float32),
            pltpu.VMEM((PASSES, BLOCK, LANES), jnp.bfloat16),
            pltpu.VMEM((rows + 8, LANES), jnp.float32),
            pltpu.VMEM((slots * GROUPS, LANES), jnp.float32),
            pltpu.VMEM((slots * GROUPS, LANES), jnp.float32),
            pltpu.VMEM((UNROLL, points, LANES), jnp.float32),
            pltpu.VMEM((components, batches, points), jnp.float32),
            pltpu.VMEM((SIDE, batches, LANES), jnp.float32),
            pltpu.VMEM((SIDE, batches, LANES), jnp.float32),
            pltpu.VMEM((2 * SIDE, NATOM, LANES), jnp.float32),
            pltpu.VMEM((SIDE, NATOM, LANES), jnp.float32),
            pltpu.VMEM((SIDE, NATOM, LANES), jnp.float32),
            pltpu.SemaphoreType.DMA((PASSES * 2 * MESSAGES + PASSES,)),
            pltpu.SemaphoreType.DMA((PASSES * 2 * MESSAGES + PASSES,)),
            pltpu.SemaphoreType.DMA((16,)),
            pltpu.SemaphoreType.DMA((16,)),
            pltpu.SemaphoreType.DMA,
        ],
        compiler_params=pltpu.CompilerParams(
            collective_id=0, has_side_effects=True, vmem_limit_bytes=48 * 2**20,
            dimension_semantics=("arbitrary", "arbitrary"),
        ),
    )(
        idx, coeffs, occupation.reshape(PASSES, GROUPS, LANES), basis_on_grid,
        harmonics.transpose(1, 0, 2), member,
    )
    return density, moments.T


def solution(mesh):
    placed = (
        P("row", "col"),
        P("col"),
        P("row", None, None),
        P("row", None),
        P("row"),
        P("row"),
        P("row", None, None),
    )
    return jax.shard_map(shards, mesh=mesh, in_specs=placed, out_specs=(P("row", "col"), P()), check_vma=False)
```

```python
import jax
import jax.numpy as jnp
from jax import lax
from jax.experimental import pallas as pl
from jax.experimental.pallas import tpu as pltpu
from jax.sharding import PartitionSpec as P

NATOM = 64
WIN = 96
LANES = 128
SIDE = 4
GROUPS = 8
PAD = GROUPS + 1
BLOCK = WIN * GROUPS
UNROLL = 4
MESH = pl.DeviceIdType.MESH
OFFSETS = ((0, 0), (-1, 0), (1, 0), (2, 0))
MESSAGES = 20


def message(number):
    if number < 2:
        return (0, 0), (1 - 2 * number, 0), None
    if number < 4:
        return (2 * number - 5, 0), (5 - 2 * number, 0), number - 2
    k, down = (number - 4) // 2 % 4, number % 2
    if number < 12:
        return OFFSETS[k], (0, 1 - 2 * down), None
    return (OFFSETS[k][0], 2 * down - 1), (0, 1 - 2 * down), down


def arrival(number):
    at, to, half = message(number)
    first, second = at[0] - to[0], at[1] - to[1]
    return (2 if first == -2 else first, 2 if second == -2 else second), half


def kernel(
    idx_ref, coeffs_ref, occ_ref, m_ref, harm_hbm, member_ref, density_ref, moments_ref,
    window, staged, other, wide, even, odd, acc, harm, part, parts, column, line, plane,
    send_sem, recv_sem, sum_send, sum_recv, harm_sem,
):
    step, steps = pl.program_id(0), pl.num_programs(0)
    me = lax.axis_index("row")
    z = lax.axis_index("col")
    y, x, core = me // (2 * SIDE), (me // 2) % SIDE, me % 2
    slots = m_ref.shape[2]
    rows = window.shape[0]

    def row_of(dy, dx):
        return (lax.rem(y + dy + SIDE, SIDE) * SIDE + lax.rem(x + dx + SIDE, SIDE)) * 2 + core

    def turned(first, second, turn):
        return first * turn + second * (1 - turn), first * (1 - turn) + second * turn

    def rows_at(at, turn, half):
        q = row_of(*turned(*at, turn)) - core + turn
        if half is None:
            return pl.ds(pl.multiple_of(q * BLOCK, BLOCK), BLOCK)
        return pl.ds(pl.multiple_of(q * BLOCK + half * (BLOCK // 2), BLOCK // 2), BLOCK // 2)

    def copy(turn, number, at, half):
        to = message(number)[1]
        place = window.at[rows_at(at, turn, half)]
        sem = turn * MESSAGES + number
        return pltpu.make_async_remote_copy(
            src_ref=place, dst_ref=place, send_sem=send_sem.at[sem], recv_sem=recv_sem.at[sem],
            device_id=(row_of(*turned(*to, turn)), z), device_id_type=MESH,
        )

    def outgoing(turn, number):
        at, _, half = message(number)
        return copy(turn, number, at, half)

    def send(turn, *numbers):
        for number in numbers:
            outgoing(turn, number).start()

    def arrive(turn, *numbers):
        for number in numbers:
            at, half = arrival(number)
            copy(turn, number, at, half).wait_recv()

    a, b = core, 1 - core
    partner = me - core + b

    def swap(turn):
        return pltpu.make_async_remote_copy(
            src_ref=other, dst_ref=window.at[rows_at((0, 0), turn, None)],
            send_sem=send_sem.at[2 * MESSAGES], recv_sem=recv_sem.at[2 * MESSAGES],
            device_id=(partner, z), device_id_type=MESH,
        )

    def outward(turn):
        send(turn, 0, 1, 4, 5)

    def first_hop(turn):
        arrive(turn, 0)
        send(turn, 2)
        arrive(turn, 1)
        send(turn, 3, 6, 7, 8, 9)

    def second_hop(turn):
        arrive(turn, 2, 3)
        send(turn, 10, 11)

    def onward(turn, k):
        arrive(turn, 4 + 2 * k)
        send(turn, 12 + 2 * k)
        arrive(turn, 5 + 2 * k)
        send(turn, 13 + 2 * k)

    def widen(turn, at):
        held = rows_at(at, turn, None)
        wide[held, :] = window[held, :].astype(jnp.float32)

    pairs = [(dz, dc) for dz in range(SIDE) for dc in range(2) if (dz, dc) != (0, 0)]

    def column_device(dz, dc):
        return me - core + lax.rem(core + dc, 2), lax.rem(z + dz, SIDE)

    def pick(into, batch, low, high):
        for s in range(low, high):
            into[pl.ds(s * PAD, GROUPS), :] = wide[pl.ds(idx_ref[batch * slots + s], GROUPS), :]

    harm_copy = pltpu.make_async_copy(harm_hbm, harm, harm_sem)

    @pl.when(step == 0)
    def _():
        harm_copy.start()
        for j in range(GROUPS):
            staged[pl.ds(j, 2 * WIN, stride=GROUPS), :] = coeffs_ref[:, j * LANES : (j + 1) * LANES].astype(
                jnp.float32
            )
        other[...] = staged[pl.ds(pl.multiple_of(b * BLOCK, BLOCK), BLOCK), :].astype(jnp.bfloat16)
        window[rows_at((0, 0), a, None), :] = staged[pl.ds(pl.multiple_of(a * BLOCK, BLOCK), BLOCK), :].astype(
            jnp.bfloat16
        )
        barrier = pltpu.get_barrier_semaphore()
        near = [column_device(*p) for p in pairs]
        near += [(row_of(0, d), z) for d in (1, 2, 3)] + [(row_of(d, 0), z) for d in (1, 2, 3)]
        for device in near:
            pl.semaphore_signal(barrier, inc=1, device_id=device, device_id_type=MESH)
        pl.semaphore_wait(barrier, len(near))
        swap(a).start()
        outward(a)
        swap(b).wait_recv()
        outward(b)
        wide[pl.ds(rows, 8), :] = jnp.zeros((8, LANES), jnp.float32)
        for turn in (a, b):
            first_hop(turn)
            onward(turn, 0)
        for turn in (a, b):
            second_hop(turn)
        for k in (1, 2, 3):
            for turn in (a, b):
                onward(turn, k)
        for turn in (a, b):
            for first, _ in OFFSETS:
                for second in (0, -1, 1):
                    widen(turn, (first, second))
        for k in range(4):
            for turn in (a, b):
                arrive(turn, 12 + 2 * k, 13 + 2 * k)
                widen(turn, (OFFSETS[k][0], 2))
        pick(even, 0, 0, slots)

    for which in range(UNROLL):
        held, into = (even, odd) if which % 2 == 0 else (odd, even)
        batch = UNROLL * step + which
        tiles = GROUPS // 2
        for tile in range(tiles):
            pick(into, batch + 1, tile * slots // tiles, (tile + 1) * slots // tiles)
            groups = (2 * tile, 2 * tile + 1)
            right = jnp.concatenate(
                [held[pl.ds(j, slots, stride=PAD), :].astype(jnp.bfloat16) for j in groups], axis=1
            )
            orbital = jnp.dot(m_ref[which], right, preferred_element_type=jnp.float32)
            first, second = orbital[:, :LANES], orbital[:, LANES:]
            term = first * first * occ_ref[groups[0] : groups[0] + 1, :]
            term += second * second * occ_ref[groups[1] : groups[1] + 1, :]
            acc[which] = term if tile == 0 else acc[which] + term
        row = jnp.sum(acc[which].T, axis=0, keepdims=True)
        for c in range(SIDE):
            part[c, pl.ds(batch, 1), :] = row[:, c * LANES : (c + 1) * LANES]

    @pl.when(step == steps - 1)
    def _():
        def remote(ref, slot, source, number, device):
            return pltpu.make_async_remote_copy(
                src_ref=source, dst_ref=ref.at[slot], send_sem=sum_send.at[number], recv_sem=sum_recv.at[number],
                device_id=device, device_id_type=MESH,
            )

        densities = [
            remote(parts, z, part.at[lax.rem(z + dz, SIDE)], 6 + dz, column_device(dz, 0)) for dz in (1, 2, 3)
        ]
        for one in densities:
            one.start()
        parts[z] = part[z]
        harm_copy.wait()
        lane = lax.broadcasted_iota(jnp.int32, (part.shape[1], LANES), 1)
        local = jnp.zeros((part.shape[1], LANES), jnp.float32)
        for l in range(harm.shape[0]):
            product = harm[l, :, :LANES] * part[0]
            for c in range(1, SIDE):
                product += harm[l, :, c * LANES : (c + 1) * LANES] * part[c]
            local = jnp.where(lane % NATOM == l, jnp.sum(product, axis=1, keepdims=True), local)
        slot = z * 2 + core
        by_atom = jnp.dot(
            member_ref[...], local, precision=lax.Precision.HIGHEST, preferred_element_type=jnp.float32
        )
        low = lax.broadcasted_iota(jnp.int32, (NATOM // 2, LANES), 1) < NATOM
        column[slot] = jnp.where(low, by_atom[: NATOM // 2], by_atom[NATOM // 2 :])
        columns = [remote(column, slot, column.at[slot], n, column_device(*p)) for n, p in enumerate(pairs)]
        for one in columns:
            one.start()
        for dz in (1, 2, 3):
            source = lax.rem(z - dz + SIDE, SIDE)
            remote(parts, source, part.at[0], 6 + dz, column_device(dz, 0)).wait_recv()
        density_ref[...] = parts[0] + parts[1] + parts[2] + parts[3]
        for n, (dz, dc) in enumerate(pairs):
            source = lax.rem(z - dz + SIDE, SIDE) * 2 + lax.rem(core + dc, 2)
            remote(column, source, column.at[source], n, column_device(dz, dc)).wait_recv()
        here = column[0]
        for s in range(1, 2 * SIDE):
            here = here + column[s]
        line[x] = here
        lines = [remote(line, x, line.at[x], 9 + d, (row_of(0, d), z)) for d in (1, 2, 3)]
        for one in lines:
            one.start()
        for d in (1, 2, 3):
            source = lax.rem(x - d + SIDE, SIDE)
            remote(line, source, line.at[source], 9 + d, (row_of(0, d), z)).wait_recv()
        plane[y] = line[0] + line[1] + line[2] + line[3]
        planes = [remote(plane, y, plane.at[y], 12 + d, (row_of(d, 0), z)) for d in (1, 2, 3)]
        for one in planes:
            one.start()
        for d in (1, 2, 3):
            source = lax.rem(y - d + SIDE, SIDE)
            remote(plane, source, plane.at[source], 12 + d, (row_of(d, 0), z)).wait_recv()
        turned_over = (plane[0] + plane[1] + plane[2] + plane[3]).T
        components = moments_ref.shape[0]
        moments_ref[:, : NATOM // 2] = turned_over[:components, :]
        moments_ref[:, NATOM // 2 :] = turned_over[NATOM : NATOM + components, :]
        for one in densities + columns + lines + planes:
            one.wait_send()
        swap(a).wait_send()
        for turn in (a, b):
            for number in range(MESSAGES):
                outgoing(turn, number).wait_send()


def shards(coeffs, occupation, basis_on_grid, basis_map, basis_count, batch_atom, harmonics):
    batches, points, slots = basis_on_grid.shape
    components = harmonics.shape[1]
    parity = lax.rem(lax.axis_index("row"), 2)
    shard = coeffs.shape[0]
    rows = 2 * SIDE * SIDE * BLOCK
    place = (basis_map // shard) * WIN + basis_map % shard - parity * WIN
    slot_ids = lax.broadcasted_iota(jnp.int32, (batches, slots), 1)
    place = jnp.where(slot_ids < basis_count[:, None], place * GROUPS, rows)
    idx = jnp.concatenate([place.reshape(-1), place[0]])
    member = (lax.broadcasted_iota(jnp.int32, (NATOM, batches), 0) == batch_atom[None, :]).astype(jnp.float32)
    density, moments = pl.pallas_call(
        kernel,
        grid=(batches // UNROLL,),
        in_specs=[
            pl.BlockSpec(memory_space=pltpu.SMEM),
            pl.BlockSpec(coeffs.shape, lambda i: (0, 0)),
            pl.BlockSpec((GROUPS, LANES), lambda i: (0, 0)),
            pl.BlockSpec((UNROLL, points, slots), lambda i: (i, 0, 0)),
            pl.BlockSpec(memory_space=pl.ANY),
            pl.BlockSpec((NATOM, batches), lambda i: (0, 0)),
        ],
        out_specs=(
            pl.BlockSpec((batches, points // SIDE), lambda i: (0, 0)),
            pl.BlockSpec((components, NATOM), lambda i: (0, 0)),
        ),
        out_shape=(
            jax.ShapeDtypeStruct((batches, points // SIDE), jnp.float32),
            jax.ShapeDtypeStruct((components, NATOM), jnp.float32),
        ),
        scratch_shapes=[
            pltpu.VMEM((rows, LANES), jnp.bfloat16),
            pltpu.VMEM((2 * BLOCK, LANES), jnp.float32),
            pltpu.VMEM((BLOCK, LANES), jnp.bfloat16),
            pltpu.VMEM((rows + 8, LANES), jnp.float32),
            pltpu.VMEM((slots * PAD + 8, LANES), jnp.float32),
            pltpu.VMEM((slots * PAD + 8, LANES), jnp.float32),
            pltpu.VMEM((UNROLL, points, LANES), jnp.float32),
            pltpu.VMEM((components, batches, points), jnp.float32),
            pltpu.VMEM((SIDE, batches, LANES), jnp.float32),
            pltpu.VMEM((SIDE, batches, LANES), jnp.float32),
            pltpu.VMEM((2 * SIDE, NATOM // 2, LANES), jnp.float32),
            pltpu.VMEM((SIDE, NATOM // 2, LANES), jnp.float32),
            pltpu.VMEM((SIDE, NATOM // 2, LANES), jnp.float32),
            pltpu.SemaphoreType.DMA((2 * MESSAGES + 1,)),
            pltpu.SemaphoreType.DMA((2 * MESSAGES + 1,)),
            pltpu.SemaphoreType.DMA((16,)),
            pltpu.SemaphoreType.DMA((16,)),
            pltpu.SemaphoreType.DMA,
        ],
        compiler_params=pltpu.CompilerParams(
            collective_id=0, has_side_effects=True, vmem_limit_bytes=60 * 2**20,
            dimension_semantics=("arbitrary",),
        ),
    )(
        idx, coeffs, occupation.reshape(GROUPS, LANES), basis_on_grid,
        harmonics.transpose(1, 0, 2), member,
    )
    return density, moments.T


def solution(mesh):
    placed = (
        P("row", "col"),
        P("col"),
        P("row", None, None),
        P("row", None),
        P("row"),
        P("row"),
        P("row", None, None),
    )
    return jax.shard_map(shards, mesh=mesh, in_specs=placed, out_specs=(P("row", "col"), P()), check_vma=False)
```

```python
import jax
import jax.numpy as jnp
from jax import lax
from jax.experimental import pallas as pl
from jax.experimental.pallas import tpu as pltpu
from jax.sharding import PartitionSpec as P

NATOM = 64
WIN = 96
LANES = 128
SIDE = 4
GROUPS = 8
PAD = GROUPS + 1
BLOCK = WIN * GROUPS
UNROLL = 4
MESH = pl.DeviceIdType.MESH
OFFSETS = ((0, 0), (-1, 0), (1, 0), (2, 0))
MESSAGES = 20


def message(number):
    if number < 2:
        return (0, 0), (1 - 2 * number, 0), None
    if number < 4:
        return (2 * number - 5, 0), (5 - 2 * number, 0), number - 2
    k, down = (number - 4) // 2 % 4, number % 2
    if number < 12:
        return OFFSETS[k], (0, 1 - 2 * down), None
    return (OFFSETS[k][0], 2 * down - 1), (0, 1 - 2 * down), down


def arrival(number):
    at, to, half = message(number)
    first, second = at[0] - to[0], at[1] - to[1]
    return (2 if first == -2 else first, 2 if second == -2 else second), half


def kernel(
    idx_ref, coeffs_ref, occ_ref, m_hbm, harm_hbm, member_ref, density_ref, moments_ref,
    window, staged, other, wide, even, odd, acc, values, harm, part, parts, column, line, plane,
    send_sem, recv_sem, sum_send, sum_recv, values_sem, harm_sem,
):
    step, steps = pl.program_id(0), pl.num_programs(0)
    me = lax.axis_index("row")
    z = lax.axis_index("col")
    y, x, core = me // (2 * SIDE), (me // 2) % SIDE, me % 2
    batches, _, slots = m_hbm.shape
    rows = window.shape[0]

    def row_of(dy, dx):
        return (lax.rem(y + dy + SIDE, SIDE) * SIDE + lax.rem(x + dx + SIDE, SIDE)) * 2 + core

    def turned(first, second, turn):
        return first * turn + second * (1 - turn), first * (1 - turn) + second * turn

    def rows_at(at, turn, half):
        q = row_of(*turned(*at, turn)) - core + turn
        if half is None:
            return pl.ds(pl.multiple_of(q * BLOCK, BLOCK), BLOCK)
        return pl.ds(pl.multiple_of(q * BLOCK + half * (BLOCK // 2), BLOCK // 2), BLOCK // 2)

    def copy(turn, number, at, half):
        to = message(number)[1]
        place = window.at[rows_at(at, turn, half)]
        sem = turn * MESSAGES + number
        return pltpu.make_async_remote_copy(
            src_ref=place, dst_ref=place, send_sem=send_sem.at[sem], recv_sem=recv_sem.at[sem],
            device_id=(row_of(*turned(*to, turn)), z), device_id_type=MESH,
        )

    def outgoing(turn, number):
        at, _, half = message(number)
        return copy(turn, number, at, half)

    def send(turn, *numbers):
        for number in numbers:
            outgoing(turn, number).start()

    def arrive(turn, *numbers):
        for number in numbers:
            at, half = arrival(number)
            copy(turn, number, at, half).wait_recv()

    a, b = core, 1 - core
    partner = me - core + b

    def swap(turn):
        return pltpu.make_async_remote_copy(
            src_ref=other, dst_ref=window.at[rows_at((0, 0), turn, None)],
            send_sem=send_sem.at[2 * MESSAGES], recv_sem=recv_sem.at[2 * MESSAGES],
            device_id=(partner, z), device_id_type=MESH,
        )

    def outward(turn):
        send(turn, 0, 1, 4, 5)

    def first_hop(turn):
        arrive(turn, 0)
        send(turn, 2)
        arrive(turn, 1)
        send(turn, 3, 6, 7, 8, 9)

    def second_hop(turn):
        arrive(turn, 2, 3)
        send(turn, 10, 11)

    def onward(turn, k):
        arrive(turn, 4 + 2 * k)
        send(turn, 12 + 2 * k)
        arrive(turn, 5 + 2 * k)
        send(turn, 13 + 2 * k)

    def widen(turn, at):
        held = rows_at(at, turn, None)
        wide[held, :] = window[held, :].astype(jnp.float32)

    pairs = [(dz, dc) for dz in range(SIDE) for dc in range(2) if (dz, dc) != (0, 0)]

    def column_device(dz, dc):
        return me - core + lax.rem(core + dc, 2), lax.rem(z + dz, SIDE)

    def pick(into, batch, low, high):
        for s in range(low, high):
            into[pl.ds(s * PAD, GROUPS), :] = wide[pl.ds(idx_ref[batch * slots + s], GROUPS), :]

    def values_copy(at, slot):
        batch = pl.multiple_of(at * UNROLL, UNROLL)
        return pltpu.make_async_copy(m_hbm.at[pl.ds(batch, UNROLL)], values.at[slot], values_sem.at[slot])

    harm_copy = pltpu.make_async_copy(harm_hbm, harm, harm_sem)

    @pl.when(step == 0)
    def _():
        barrier = pltpu.get_barrier_semaphore()
        near = [column_device(*p) for p in pairs]
        near += [(row_of(0, d), z) for d in (1, 2, 3)] + [(row_of(d, 0), z) for d in (1, 2, 3)]
        for device in near:
            pl.semaphore_signal(barrier, inc=1, device_id=device, device_id_type=MESH)
        values_copy(0, 0).start()
        for j in range(GROUPS):
            staged[pl.ds(j, 2 * WIN, stride=GROUPS), :] = coeffs_ref[:, j * LANES : (j + 1) * LANES].astype(
                jnp.float32
            )
        other[...] = staged[pl.ds(pl.multiple_of(b * BLOCK, BLOCK), BLOCK), :].astype(jnp.bfloat16)
        window[rows_at((0, 0), a, None), :] = staged[pl.ds(pl.multiple_of(a * BLOCK, BLOCK), BLOCK), :].astype(
            jnp.bfloat16
        )
        wide[pl.ds(rows, 8), :] = jnp.zeros((8, LANES), jnp.float32)
        pl.semaphore_wait(barrier, len(near))
        swap(a).start()
        outward(a)
        swap(b).wait_recv()
        outward(b)
        harm_copy.start()
        for turn in (a, b):
            first_hop(turn)
            onward(turn, 0)
        for turn in (a, b):
            second_hop(turn)
        for k in (1, 2, 3):
            for turn in (a, b):
                onward(turn, k)
        for turn in (a, b):
            for first, _ in OFFSETS:
                for second in (0, -1, 1):
                    widen(turn, (first, second))
        for k in range(4):
            for turn in (a, b):
                arrive(turn, 12 + 2 * k, 13 + 2 * k)
                widen(turn, (OFFSETS[k][0], 2))
        pick(even, 0, 0, slots)

    turn_of = lax.rem(step, 2)
    values_copy(step, turn_of).wait()

    @pl.when(step + 1 < steps)
    def _():
        values_copy(step + 1, 1 - turn_of).start()

    for which in range(UNROLL):
        held, into = (even, odd) if which % 2 == 0 else (odd, even)
        batch = UNROLL * step + which
        after = jnp.minimum(batch + 1, batches - 1)
        tiles = GROUPS // 2
        for tile in range(tiles):
            pick(into, after, tile * slots // tiles, (tile + 1) * slots // tiles)
            groups = (2 * tile, 2 * tile + 1)
            right = jnp.concatenate(
                [held[pl.ds(j, slots, stride=PAD), :].astype(jnp.bfloat16) for j in groups], axis=1
            )
            orbital = jnp.dot(values[turn_of, which], right, preferred_element_type=jnp.float32)
            first, second = orbital[:, :LANES], orbital[:, LANES:]
            term = first * first * occ_ref[groups[0] : groups[0] + 1, :]
            term += second * second * occ_ref[groups[1] : groups[1] + 1, :]
            acc[which] = term if tile == 0 else acc[which] + term
        row = jnp.sum(acc[which].T, axis=0, keepdims=True)
        for c in range(SIDE):
            part[c, pl.ds(batch, 1), :] = row[:, c * LANES : (c + 1) * LANES]

    @pl.when(step == steps - 1)
    def _():
        def remote(ref, slot, source, number, device):
            return pltpu.make_async_remote_copy(
                src_ref=source, dst_ref=ref.at[slot], send_sem=sum_send.at[number], recv_sem=sum_recv.at[number],
                device_id=device, device_id_type=MESH,
            )

        densities = [
            remote(parts, z, part.at[lax.rem(z + dz, SIDE)], 6 + dz, column_device(dz, 0)) for dz in (1, 2, 3)
        ]
        for one in densities:
            one.start()
        parts[z] = part[z]
        harm_copy.wait()
        lane = lax.broadcasted_iota(jnp.int32, (part.shape[1], LANES), 1)
        local = jnp.zeros((part.shape[1], LANES), jnp.float32)
        for l in range(harm.shape[0]):
            product = harm[l, :, :LANES] * part[0]
            for c in range(1, SIDE):
                product += harm[l, :, c * LANES : (c + 1) * LANES] * part[c]
            local = jnp.where(lane % NATOM == l, jnp.sum(product, axis=1, keepdims=True), local)
        slot = z * 2 + core
        by_atom = jnp.dot(
            member_ref[...], local, precision=lax.Precision.HIGHEST, preferred_element_type=jnp.float32
        )
        low = lax.broadcasted_iota(jnp.int32, (NATOM // 2, LANES), 1) < NATOM
        column[slot] = jnp.where(low, by_atom[: NATOM // 2], by_atom[NATOM // 2 :])
        columns = [remote(column, slot, column.at[slot], n, column_device(*p)) for n, p in enumerate(pairs)]
        for one in columns:
            one.start()
        for dz in (1, 2, 3):
            source = lax.rem(z - dz + SIDE, SIDE)
            remote(parts, source, part.at[0], 6 + dz, column_device(dz, 0)).wait_recv()
        density_ref[...] = parts[0] + parts[1] + parts[2] + parts[3]
        for n, (dz, dc) in enumerate(pairs):
            source = lax.rem(z - dz + SIDE, SIDE) * 2 + lax.rem(core + dc, 2)
            remote(column, source, column.at[source], n, column_device(dz, dc)).wait_recv()
        here = column[0]
        for s in range(1, 2 * SIDE):
            here = here + column[s]
        line[x] = here
        lines = [remote(line, x, line.at[x], 9 + d, (row_of(0, d), z)) for d in (1, 2, 3)]
        for one in lines:
            one.start()
        for d in (1, 2, 3):
            source = lax.rem(x - d + SIDE, SIDE)
            remote(line, source, line.at[source], 9 + d, (row_of(0, d), z)).wait_recv()
        plane[y] = line[0] + line[1] + line[2] + line[3]
        planes = [remote(plane, y, plane.at[y], 12 + d, (row_of(d, 0), z)) for d in (1, 2, 3)]
        for one in planes:
            one.start()
        for d in (1, 2, 3):
            source = lax.rem(y - d + SIDE, SIDE)
            remote(plane, source, plane.at[source], 12 + d, (row_of(d, 0), z)).wait_recv()
        turned_over = (plane[0] + plane[1] + plane[2] + plane[3]).T
        components = moments_ref.shape[0]
        moments_ref[:, : NATOM // 2] = turned_over[:components, :]
        moments_ref[:, NATOM // 2 :] = turned_over[NATOM : NATOM + components, :]
        for one in densities + columns + lines + planes:
            one.wait_send()
        swap(a).wait_send()
        for turn in (a, b):
            for number in range(MESSAGES):
                outgoing(turn, number).wait_send()


def shards(coeffs, occupation, basis_on_grid, basis_map, basis_count, batch_atom, harmonics):
    batches, points, slots = basis_on_grid.shape
    components = harmonics.shape[1]
    parity = lax.rem(lax.axis_index("row"), 2)
    shard = coeffs.shape[0]
    rows = 2 * SIDE * SIDE * BLOCK
    place = (basis_map // shard) * WIN + basis_map % shard - parity * WIN
    slot_ids = lax.broadcasted_iota(jnp.int32, (batches, slots), 1)
    place = jnp.where(slot_ids < basis_count[:, None], place * GROUPS, rows)
    idx = place.reshape(-1)
    member = (lax.broadcasted_iota(jnp.int32, (NATOM, batches), 0) == batch_atom[None, :]).astype(jnp.float32)
    density, moments = pl.pallas_call(
        kernel,
        grid=(batches // UNROLL,),
        in_specs=[
            pl.BlockSpec(memory_space=pltpu.SMEM),
            pl.BlockSpec(coeffs.shape, lambda i: (0, 0)),
            pl.BlockSpec((GROUPS, LANES), lambda i: (0, 0)),
            pl.BlockSpec(memory_space=pltpu.HBM),
            pl.BlockSpec(memory_space=pltpu.HBM),
            pl.BlockSpec((NATOM, batches), lambda i: (0, 0)),
        ],
        out_specs=(
            pl.BlockSpec((batches, points // SIDE), lambda i: (0, 0)),
            pl.BlockSpec((components, NATOM), lambda i: (0, 0)),
        ),
        out_shape=(
            jax.ShapeDtypeStruct((batches, points // SIDE), jnp.float32),
            jax.ShapeDtypeStruct((components, NATOM), jnp.float32),
        ),
        scratch_shapes=[
            pltpu.VMEM((rows, LANES), jnp.bfloat16),
            pltpu.VMEM((2 * BLOCK, LANES), jnp.float32),
            pltpu.VMEM((BLOCK, LANES), jnp.bfloat16),
            pltpu.VMEM((rows + 8, LANES), jnp.float32),
            pltpu.VMEM((slots * PAD + 8, LANES), jnp.float32),
            pltpu.VMEM((slots * PAD + 8, LANES), jnp.float32),
            pltpu.VMEM((UNROLL, points, LANES), jnp.float32),
            pltpu.VMEM((2, UNROLL, points, slots), jnp.bfloat16),
            pltpu.VMEM((components, batches, points), jnp.float32),
            pltpu.VMEM((SIDE, batches, LANES), jnp.float32),
            pltpu.VMEM((SIDE, batches, LANES), jnp.float32),
            pltpu.VMEM((2 * SIDE, NATOM // 2, LANES), jnp.float32),
            pltpu.VMEM((SIDE, NATOM // 2, LANES), jnp.float32),
            pltpu.VMEM((SIDE, NATOM // 2, LANES), jnp.float32),
            pltpu.SemaphoreType.DMA((2 * MESSAGES + 1,)),
            pltpu.SemaphoreType.DMA((2 * MESSAGES + 1,)),
            pltpu.SemaphoreType.DMA((16,)),
            pltpu.SemaphoreType.DMA((16,)),
            pltpu.SemaphoreType.DMA((2,)),
            pltpu.SemaphoreType.DMA,
        ],
        compiler_params=pltpu.CompilerParams(
            collective_id=0, has_side_effects=True, vmem_limit_bytes=52 * 2**20,
            dimension_semantics=("arbitrary",),
        ),
    )(
        idx, coeffs, occupation.reshape(GROUPS, LANES), basis_on_grid,
        harmonics.transpose(1, 0, 2), member,
    )
    return density, moments.T


def solution(mesh):
    placed = (
        P("row", "col"),
        P("col"),
        P("row", None, None),
        P("row", None),
        P("row"),
        P("row"),
        P("row", None, None),
    )
    return jax.shard_map(shards, mesh=mesh, in_specs=placed, out_specs=(P("row", "col"), P()), check_vma=False)
```

```python
import jax
import jax.numpy as jnp
from jax import lax
from jax.experimental import pallas as pl
from jax.experimental.pallas import tpu as pltpu
from jax.sharding import PartitionSpec as P

NATOM = 64
WIN = 96
LANES = 128
SIDE = 4
GROUPS = 8
TILE = 4
PAD = GROUPS + 1
BLOCK = WIN * GROUPS
UNROLL = 4
MESH = pl.DeviceIdType.MESH
OFFSETS = ((0, 0), (-1, 0), (1, 0), (2, 0))
MESSAGES = 20


def message(number):
    if number < 2:
        return (0, 0), (1 - 2 * number, 0), None
    if number < 4:
        return (2 * number - 5, 0), (5 - 2 * number, 0), number - 2
    k, down = (number - 4) // 2 % 4, number % 2
    if number < 12:
        return OFFSETS[k], (0, 1 - 2 * down), None
    return (OFFSETS[k][0], 2 * down - 1), (0, 1 - 2 * down), down


def arrival(number):
    at, to, half = message(number)
    first, second = at[0] - to[0], at[1] - to[1]
    return (2 if first == -2 else first, 2 if second == -2 else second), half


def kernel(
    idx_ref, coeffs_ref, occ_ref, m_hbm, harm_hbm, member_ref, density_ref, moments_ref,
    window, staged, other, wide, even, odd, acc, values, harm, part, parts, column, line, plane,
    send_sem, recv_sem, sum_send, sum_recv, values_sem, harm_sem,
):
    step, steps = pl.program_id(0), pl.num_programs(0)
    me = lax.axis_index("row")
    z = lax.axis_index("col")
    y, x, core = me // (2 * SIDE), (me // 2) % SIDE, me % 2
    batches, _, slots = m_hbm.shape
    rows = window.shape[0]

    def row_of(dy, dx):
        return (lax.rem(y + dy + SIDE, SIDE) * SIDE + lax.rem(x + dx + SIDE, SIDE)) * 2 + core

    def turned(first, second, turn):
        return first * turn + second * (1 - turn), first * (1 - turn) + second * turn

    def rows_at(at, turn, half):
        q = row_of(*turned(*at, turn)) - core + turn
        if half is None:
            return pl.ds(pl.multiple_of(q * BLOCK, BLOCK), BLOCK)
        return pl.ds(pl.multiple_of(q * BLOCK + half * (BLOCK // 2), BLOCK // 2), BLOCK // 2)

    def copy(turn, number, at, half):
        to = message(number)[1]
        place = window.at[rows_at(at, turn, half)]
        sem = turn * MESSAGES + number
        return pltpu.make_async_remote_copy(
            src_ref=place, dst_ref=place, send_sem=send_sem.at[sem], recv_sem=recv_sem.at[sem],
            device_id=(row_of(*turned(*to, turn)), z), device_id_type=MESH,
        )

    def outgoing(turn, number):
        at, _, half = message(number)
        return copy(turn, number, at, half)

    def send(turn, *numbers):
        for number in numbers:
            outgoing(turn, number).start()

    def arrive(turn, *numbers):
        for number in numbers:
            at, half = arrival(number)
            copy(turn, number, at, half).wait_recv()

    a, b = core, 1 - core
    partner = me - core + b

    def swap(turn):
        return pltpu.make_async_remote_copy(
            src_ref=other, dst_ref=window.at[rows_at((0, 0), turn, None)],
            send_sem=send_sem.at[2 * MESSAGES], recv_sem=recv_sem.at[2 * MESSAGES],
            device_id=(partner, z), device_id_type=MESH,
        )

    def outward(turn):
        send(turn, 0, 1, 4, 5)

    def first_hop(turn):
        arrive(turn, 0)
        send(turn, 2)
        arrive(turn, 1)
        send(turn, 3, 6, 7, 8, 9)

    def second_hop(turn):
        arrive(turn, 2, 3)
        send(turn, 10, 11)

    def onward(turn, k):
        arrive(turn, 4 + 2 * k)
        send(turn, 12 + 2 * k)
        arrive(turn, 5 + 2 * k)
        send(turn, 13 + 2 * k)

    def widen(turn, at):
        held = rows_at(at, turn, None)
        wide[held, :] = window[held, :].astype(jnp.float32)

    pairs = [(dz, dc) for dz in range(SIDE) for dc in range(2) if (dz, dc) != (0, 0)]

    def column_device(dz, dc):
        return me - core + lax.rem(core + dc, 2), lax.rem(z + dz, SIDE)

    def pick(into, batch, low, high):
        for s in range(low, high):
            into[pl.ds(s * PAD, GROUPS), :] = wide[pl.ds(idx_ref[batch * slots + s], GROUPS), :]

    def values_copy(at, slot):
        batch = pl.multiple_of(at * UNROLL, UNROLL)
        return pltpu.make_async_copy(m_hbm.at[pl.ds(batch, UNROLL)], values.at[slot], values_sem.at[slot])

    harm_copy = pltpu.make_async_copy(harm_hbm, harm, harm_sem)

    @pl.when(step == 0)
    def _():
        barrier = pltpu.get_barrier_semaphore()
        near = [column_device(*p) for p in pairs]
        near += [(row_of(0, d), z) for d in (1, 2, 3)] + [(row_of(d, 0), z) for d in (1, 2, 3)]
        for device in near:
            pl.semaphore_signal(barrier, inc=1, device_id=device, device_id_type=MESH)
        values_copy(0, 0).start()
        for j in range(GROUPS):
            staged[pl.ds(j, 2 * WIN, stride=GROUPS), :] = coeffs_ref[:, j * LANES : (j + 1) * LANES].astype(
                jnp.float32
            )
        other[...] = staged[pl.ds(pl.multiple_of(b * BLOCK, BLOCK), BLOCK), :].astype(jnp.bfloat16)
        window[rows_at((0, 0), a, None), :] = staged[pl.ds(pl.multiple_of(a * BLOCK, BLOCK), BLOCK), :].astype(
            jnp.bfloat16
        )
        wide[pl.ds(rows, 8), :] = jnp.zeros((8, LANES), jnp.float32)
        pl.semaphore_wait(barrier, len(near))
        swap(a).start()
        outward(a)
        swap(b).wait_recv()
        outward(b)
        harm_copy.start()
        for turn in (a, b):
            first_hop(turn)
            onward(turn, 0)
        for turn in (a, b):
            second_hop(turn)
        for k in (1, 2, 3):
            for turn in (a, b):
                onward(turn, k)
        for turn in (a, b):
            for first, _ in OFFSETS:
                for second in (0, -1, 1):
                    widen(turn, (first, second))
        for k in range(4):
            for turn in (a, b):
                arrive(turn, 12 + 2 * k, 13 + 2 * k)
                widen(turn, (OFFSETS[k][0], 2))
        pick(even, 0, 0, slots)

    turn_of = lax.rem(step, 2)
    none = jnp.minimum(step, 0)
    spare, zeros = pl.ds(slots * PAD + none, 8), pl.ds(rows + none, 8)
    values_copy(step, turn_of).wait()

    @pl.when(step + 1 < steps)
    def _():
        values_copy(step + 1, 1 - turn_of).start()

    for which in range(UNROLL):
        held, into = (even, odd) if which % 2 == 0 else (odd, even)
        batch = UNROLL * step + which
        after = jnp.minimum(batch + 1, batches - 1)
        tiles = GROUPS // TILE
        for tile in range(tiles):
            pick(into, after, tile * slots // tiles, (tile + 1) * slots // tiles)
            groups = range(TILE * tile, TILE * (tile + 1))
            right = jnp.concatenate(
                [held[pl.ds(j, slots, stride=PAD), :].astype(jnp.bfloat16) for j in groups], axis=1
            )
            orbital = jnp.dot(values[turn_of, which], right, preferred_element_type=jnp.float32)
            term = None
            for n, j in enumerate(groups):
                one = orbital[:, n * LANES : (n + 1) * LANES]
                square = one * one * occ_ref[j : j + 1, :]
                term = square if term is None else term + square
            acc[which] = term if tile == 0 else acc[which] + term
            held[spare, :] = jnp.zeros((8, LANES), jnp.float32)
            wide[zeros, :] = held[spare, :]
            held[spare, :] = wide[zeros, :]
        row = jnp.sum(acc[which].T, axis=0, keepdims=True)
        for c in range(SIDE):
            part[c, pl.ds(batch, 1), :] = row[:, c * LANES : (c + 1) * LANES]

    @pl.when(step == steps - 1)
    def _():
        def remote(ref, slot, source, number, device):
            return pltpu.make_async_remote_copy(
                src_ref=source, dst_ref=ref.at[slot], send_sem=sum_send.at[number], recv_sem=sum_recv.at[number],
                device_id=device, device_id_type=MESH,
            )

        densities = [
            remote(parts, z, part.at[lax.rem(z + dz, SIDE)], 6 + dz, column_device(dz, 0)) for dz in (1, 2, 3)
        ]
        harm_copy.wait()
        lane = lax.broadcasted_iota(jnp.int32, (part.shape[1], LANES), 1)
        local = jnp.zeros((part.shape[1], LANES), jnp.float32)
        for l in range(harm.shape[0]):
            product = harm[l, :, :LANES] * part[0]
            for c in range(1, SIDE):
                product += harm[l, :, c * LANES : (c + 1) * LANES] * part[c]
            local = jnp.where(lane % NATOM == l, jnp.sum(product, axis=1, keepdims=True), local)
        slot = z * 2 + core
        by_atom = jnp.dot(
            member_ref[...], local, precision=lax.Precision.HIGHEST, preferred_element_type=jnp.float32
        )
        low = lax.broadcasted_iota(jnp.int32, (NATOM // 2, LANES), 1) < NATOM
        column[slot] = jnp.where(low, by_atom[: NATOM // 2], by_atom[NATOM // 2 :])
        columns = [remote(column, slot, column.at[slot], n, column_device(*p)) for n, p in enumerate(pairs)]
        for one in columns:
            one.start()
        for one in densities:
            one.start()
        parts[z] = part[z]
        for n, (dz, dc) in enumerate(pairs):
            source = lax.rem(z - dz + SIDE, SIDE) * 2 + lax.rem(core + dc, 2)
            remote(column, source, column.at[source], n, column_device(dz, dc)).wait_recv()
        here = column[0]
        for s in range(1, 2 * SIDE):
            here = here + column[s]
        line[x] = here
        lines = [remote(line, x, line.at[x], 9 + d, (row_of(0, d), z)) for d in (1, 2, 3)]
        for one in lines:
            one.start()
        for dz in (1, 2, 3):
            source = lax.rem(z - dz + SIDE, SIDE)
            remote(parts, source, part.at[0], 6 + dz, column_device(dz, 0)).wait_recv()
        density_ref[...] = parts[0] + parts[1] + parts[2] + parts[3]
        for d in (1, 2, 3):
            source = lax.rem(x - d + SIDE, SIDE)
            remote(line, source, line.at[source], 9 + d, (row_of(0, d), z)).wait_recv()
        plane[y] = line[0] + line[1] + line[2] + line[3]
        planes = [remote(plane, y, plane.at[y], 12 + d, (row_of(d, 0), z)) for d in (1, 2, 3)]
        for one in planes:
            one.start()
        for d in (1, 2, 3):
            source = lax.rem(y - d + SIDE, SIDE)
            remote(plane, source, plane.at[source], 12 + d, (row_of(d, 0), z)).wait_recv()
        turned_over = (plane[0] + plane[1] + plane[2] + plane[3]).T
        components = moments_ref.shape[0]
        moments_ref[:, : NATOM // 2] = turned_over[:components, :]
        moments_ref[:, NATOM // 2 :] = turned_over[NATOM : NATOM + components, :]
        for one in densities + columns + lines + planes:
            one.wait_send()
        swap(a).wait_send()
        for turn in (a, b):
            for number in range(MESSAGES):
                outgoing(turn, number).wait_send()


def shards(coeffs, occupation, basis_on_grid, basis_map, basis_count, batch_atom, harmonics):
    batches, points, slots = basis_on_grid.shape
    components = harmonics.shape[1]
    parity = lax.rem(lax.axis_index("row"), 2)
    shard = coeffs.shape[0]
    rows = 2 * SIDE * SIDE * BLOCK
    place = (basis_map // shard) * WIN + basis_map % shard - parity * WIN
    slot_ids = lax.broadcasted_iota(jnp.int32, (batches, slots), 1)
    place = jnp.where(slot_ids < basis_count[:, None], place * GROUPS, rows)
    idx = place.reshape(-1)
    member = (lax.broadcasted_iota(jnp.int32, (NATOM, batches), 0) == batch_atom[None, :]).astype(jnp.float32)
    density, moments = pl.pallas_call(
        kernel,
        grid=(batches // UNROLL,),
        in_specs=[
            pl.BlockSpec(memory_space=pltpu.SMEM),
            pl.BlockSpec(coeffs.shape, lambda i: (0, 0)),
            pl.BlockSpec((GROUPS, LANES), lambda i: (0, 0)),
            pl.BlockSpec(memory_space=pltpu.HBM),
            pl.BlockSpec(memory_space=pltpu.HBM),
            pl.BlockSpec((NATOM, batches), lambda i: (0, 0)),
        ],
        out_specs=(
            pl.BlockSpec((batches, points // SIDE), lambda i: (0, 0)),
            pl.BlockSpec((components, NATOM), lambda i: (0, 0)),
        ),
        out_shape=(
            jax.ShapeDtypeStruct((batches, points // SIDE), jnp.float32),
            jax.ShapeDtypeStruct((components, NATOM), jnp.float32),
        ),
        scratch_shapes=[
            pltpu.VMEM((rows, LANES), jnp.bfloat16),
            pltpu.VMEM((2 * BLOCK, LANES), jnp.float32),
            pltpu.VMEM((BLOCK, LANES), jnp.bfloat16),
            pltpu.VMEM((rows + 8, LANES), jnp.float32),
            pltpu.VMEM((slots * PAD + 8, LANES), jnp.float32),
            pltpu.VMEM((slots * PAD + 8, LANES), jnp.float32),
            pltpu.VMEM((UNROLL, points, LANES), jnp.float32),
            pltpu.VMEM((2, UNROLL, points, slots), jnp.bfloat16),
            pltpu.VMEM((components, batches, points), jnp.float32),
            pltpu.VMEM((SIDE, batches, LANES), jnp.float32),
            pltpu.VMEM((SIDE, batches, LANES), jnp.float32),
            pltpu.VMEM((2 * SIDE, NATOM // 2, LANES), jnp.float32),
            pltpu.VMEM((SIDE, NATOM // 2, LANES), jnp.float32),
            pltpu.VMEM((SIDE, NATOM // 2, LANES), jnp.float32),
            pltpu.SemaphoreType.DMA((2 * MESSAGES + 1,)),
            pltpu.SemaphoreType.DMA((2 * MESSAGES + 1,)),
            pltpu.SemaphoreType.DMA((16,)),
            pltpu.SemaphoreType.DMA((16,)),
            pltpu.SemaphoreType.DMA((2,)),
            pltpu.SemaphoreType.DMA,
        ],
        compiler_params=pltpu.CompilerParams(
            collective_id=0, has_side_effects=True, vmem_limit_bytes=52 * 2**20,
            dimension_semantics=("arbitrary",),
        ),
    )(
        idx, coeffs, occupation.reshape(GROUPS, LANES), basis_on_grid,
        harmonics.transpose(1, 0, 2), member,
    )
    return density, moments.T


def solution(mesh):
    placed = (
        P("row", "col"),
        P("col"),
        P("row", None, None),
        P("row", None),
        P("row"),
        P("row"),
        P("row", None, None),
    )
    return jax.shard_map(shards, mesh=mesh, in_specs=placed, out_specs=(P("row", "col"), P()), check_vma=False)
```
